32 devices in a mesh: groups: 2 (over y), freq: 16 (over z, x, core).
Axes of the slice: x: 2, y: 2, z: 4, core: 2. Of those that a mesh axis runs over, the one named last changes fastest.
Arguments:
- primary_one: bfloat16 [1024, 512, 512], P(('groups', 'freq')), parts along dimension 0, may hold values from -6 to 6
- primary_two: bfloat16 [1024, 512, 512], P(('groups', 'freq')), parts along dimension 0, may hold values from -6 to 6
- primary_three: bfloat16 [1024, 512, 512], P(('groups', 'freq')), parts along dimension 0, may hold values from -6 to 6
- window_start: int32 [3, 1024, 512], P(None, ('groups', 'freq')), parts along dimension 1, may hold values from 0 to 255
- window_end: int32 [3, 1024, 512], P(None, ('groups', 'freq')), parts along dimension 1, may hold values from 257 to 512
Outputs:
- predicted: bfloat16 [1024, 512, 512], P(('groups', 'freq')), parts along dimension 0
The draws below stay inside these ranges and needn't reach their ends.
There are 2 independent parts, one for each index of `groups`. The reference program is written for one: setup_inputs(seed, part) draws one part's arguments, and reference() takes and returns one part's arrays. A program takes and returns all parts, laid end to end along the dimension named above; each array names one. Nothing has to cross between parts.
Inputs may be any that keep to these rules, and one draw needn't show every extreme that they name: window_start of a trace is below its window_end.
All inputs are finite; a program needn't handle non-finite values.
Results may differ from the reference program's by a relative error of at most 0.0089.
Values may be sent and summed in bfloat16 or wider, within the bound.
A program may use at most 128 MiB of HBM per device.

```python
import jax
import jax.numpy as jnp
from jax import lax

NS = 512
NR = 512
NT = 512
NF = 16


def touch_ends(result, stream_key, least, high):
    index_at = [jax.random.randint(jax.random.fold_in(stream_key, axis), (), 0, length) for axis, length in enumerate(result.shape)]
    widest = result.shape.index(max(result.shape))
    beside = index_at[:widest] + [(index_at[widest] + 1) % result.shape[widest]] + index_at[widest + 1:]
    return result.at[tuple(index_at)].set(least).at[tuple(beside)].set(high)


def steps_of(stream_key, shape, cuts, low, largest):
    level = 1.0
    for dim, parts in cuts:
        steps = jax.random.uniform(jax.random.fold_in(jax.random.fold_in(stream_key, 6), dim), (parts,), jnp.float32, low / len(cuts), largest / len(cuts))
        level = level * jnp.repeat(jnp.exp(steps), shape[dim] // parts).reshape((-1,) + (1,) * (len(shape) - 1 - dim))
    return level


def centred(stream_key, shape, spread, reach, pieces=(), kind=jnp.bfloat16):
    gain = steps_of(stream_key, shape, pieces, -0.22, 0.18) if pieces else 1.0
    entries = jax.random.normal(stream_key, shape, jnp.float32) * spread * gain
    return jnp.minimum(jnp.maximum(entries, -reach), reach).astype(kind)


def setup_inputs(seed: int = 0, part: int = 0) -> dict:
    streams_of = jax.random.split(jax.random.key(seed), 6)
    part_splits = jax.random.split(jax.random.fold_in(streams_of[5], part), 6)
    return {
        "primary_one": centred(part_splits[0], (NS, NR, NT), 1.0, 6.0, ((0, 16),)),
        "primary_two": centred(part_splits[1], (NS, NR, NT), 1.0, 6.0, ((0, 16),)),
        "primary_three": centred(part_splits[2], (NS, NR, NT), 1.0, 6.0, ((0, 16),)),
        "window_start": touch_ends(jax.random.randint(part_splits[3], (3, NS, NR), 0, NT // 2), jax.random.fold_in(part_splits[3], 1), 0, (NT // 2) - 1).astype(jnp.int32),
        "window_end": touch_ends(jax.random.randint(part_splits[4], (3, NS, NR), NT // 2 + 1, NT + 1), jax.random.fold_in(part_splits[4], 1), NT // 2 + 1, NT).astype(jnp.int32),
    }


def make_table(count, samples):
    waves = jnp.arange(1, count + 1, dtype=jnp.int32)[:, None]
    times = jnp.arange(samples, dtype=jnp.int32)[None, :]
    phase = waves * times % samples
    angle = 2.0 * jnp.pi / samples * phase.astype(jnp.float32)
    both = jnp.stack([jnp.cos(angle), -jnp.sin(angle)], axis=1)
    return both.reshape(2 * count, samples).astype(jnp.bfloat16)

def spectrum(traces, start, finish, table):
    times = jnp.arange(NT, dtype=jnp.int32)
    inside = (times >= start[:, :, None]) & (times < finish[:, :, None])
    windowed = jnp.where(inside, traces, jnp.zeros_like(traces))
    flat = windowed.reshape(NS * NR, NT)
    spec = lax.dot_general(table, flat, (((1,), (1,)), ((), ())), preferred_element_type=jnp.float32)
    spec = spec * (1.0 / jnp.sqrt(jnp.float32(NT)))
    return spec.astype(jnp.bfloat16).reshape(NF, 2, NS, NR)

def slice_product(items):
    first, second, third = items
    first = first.astype(jnp.float32)
    second = second.astype(jnp.float32)
    third = third.astype(jnp.float32)
    high = lax.Precision.HIGHEST
    cross_re = jnp.dot(first[0], second[0].T, precision=high) + jnp.dot(first[1], second[1].T, precision=high)
    cross_im = jnp.dot(first[1], second[0].T, precision=high) - jnp.dot(first[0], second[1].T, precision=high)
    cross = (jnp.stack([cross_re, cross_im]) * (1.0 / jnp.sqrt(jnp.float32(NR)))).astype(jnp.bfloat16)
    cross = cross.astype(jnp.float32)
    mult_re = jnp.dot(cross[0], third[0], precision=high) - jnp.dot(cross[1], third[1], precision=high)
    mult_im = jnp.dot(cross[0], third[1], precision=high) + jnp.dot(cross[1], third[0], precision=high)
    return (jnp.stack([mult_re, mult_im]) * (1.0 / jnp.sqrt(jnp.float32(NS)))).astype(jnp.bfloat16)

def reference(primary_one, primary_two, primary_three, window_start, window_end):
    table = make_table(NF, NT)
    spec_one = spectrum(primary_one, window_start[0], window_end[0], table)
    spec_two = spectrum(primary_two, window_start[1], window_end[1], table)
    spec_three = spectrum(primary_three, window_start[2], window_end[2], table)
    multiple = lax.map(slice_product, (spec_one, spec_two, spec_three))
    flat = multiple.reshape(2 * NF, NS * NR)
    timed = lax.dot_general(flat, table, (((0,), (0,)), ((), ())), preferred_element_type=jnp.float32)
    timed = timed * (1.0 / jnp.sqrt(jnp.float32(NF)))
    return timed.astype(jnp.bfloat16).reshape(NS, NR, NT)
```

```python
import functools
import math

import jax
import jax.numpy as jnp
import numpy as np
from jax import lax
from jax.experimental import pallas as pl
from jax.experimental.pallas import tpu as pltpu
from jax.sharding import PartitionSpec as P

F_DEV = 1
CHUNK = 8
PAIR = 2 * CHUNK
SUB = 2
SLOTS = 4
LANES = 128


def make_table(count, samples):
    waves = jnp.arange(1, count + 1, dtype=jnp.int32)[:, None]
    times = jnp.arange(samples, dtype=jnp.int32)[None, :]
    phase = waves * times % samples
    angle = 2.0 * jnp.pi / samples * phase.astype(jnp.float32)
    both = jnp.stack([jnp.cos(angle), -jnp.sin(angle)], axis=1)
    return both.reshape(2 * count, samples).astype(jnp.bfloat16)


def host_table(count, samples):
    waves = np.arange(1, count + 1, dtype=np.int64)[:, None]
    times = np.arange(samples, dtype=np.int64)[None, :]
    phase = waves * times % samples
    angle = np.float32(2.0 * np.pi / samples) * phase.astype(np.float32)
    both = np.stack([np.cos(angle), -np.sin(angle)], axis=1)
    return jnp.asarray(both.reshape(2 * count, samples).astype(jnp.bfloat16))


def drain(ref, sem):
    pltpu.make_async_copy(ref, ref, sem).wait()


def exchange_kernel(
    n, one_ref, two_ref, three_ref, start_hbm, end_hbm, table_hbm,
    early_ref, last_ref, wide_ref,
    start_ref, end_ref, table_ref, buf, scr, stage, r1, r2, r3, r3s, gw, mbuf, piece, turned,
    load_sem, small_sem, send_sem, r1_sem, r23_sem, out_sem,
):
    me = lax.axis_index("freq")
    sources, receivers, samples = one_ref.shape
    half = n // 2
    side = me // half
    chunks = sources // CHUNK
    total = sources // SUB
    waves = 2 * n
    middle = samples // 2
    bf = jnp.bfloat16
    f32 = jnp.float32

    def peer_far(q):
        return (1 - side) * half + lax.rem(me + q, half)

    def peer_near(q):
        return side * half + lax.rem(me + q, half)

    barrier = pltpu.get_barrier_semaphore()

    @pl.loop(1, n)
    def _(q):
        pl.semaphore_signal(
            barrier, inc=1, device_id={"freq": lax.rem(me + q, n)},
            device_id_type=pl.DeviceIdType.MESH,
        )

    sets = ((two_ref, 1, r2), (three_ref, 2, r3), (one_ref, 0, r1))

    def load(ref, i):
        slot = lax.rem(i, SLOTS)
        return pltpu.make_async_copy(
            ref.at[pl.ds(i * SUB, SUB)], buf.at[slot], load_sem.at[slot]
        )

    smalls = (
        pltpu.make_async_copy(start_hbm, start_ref, small_sem.at[0]),
        pltpu.make_async_copy(end_hbm, end_ref, small_sem.at[1]),
        pltpu.make_async_copy(table_hbm, table_ref, small_sem.at[2]),
    )
    load(sets[0][0], 0).start()
    for copy in smalls:
        copy.start()
    for i in range(1, SLOTS - 1):
        load(sets[0][0], i).start()
    for copy in smalls:
        copy.wait()

    scale_t = 1.0 / (samples ** 0.5)
    lane = lax.broadcasted_iota(jnp.int32, (receivers, LANES), 1).astype(f32)
    ticks = [(lane + c * LANES).astype(bf) for c in range(middle // LANES)]

    def column(row):
        row = jnp.broadcast_to(row.astype(f32), (LANES, receivers))
        return row.astype(bf).T

    def send(src, dst, sem, arrive, order):
        def one(p):
            pltpu.make_async_remote_copy(
                src_ref=src(p), dst_ref=dst, send_sem=sem, recv_sem=arrive,
                device_id={"freq": p}, device_id_type=pl.DeviceIdType.MESH,
            ).start()

        def far():
            @pl.loop(0, half)
            def _(q):
                one(peer_far(q))

        def near():
            pltpu.make_async_copy(src(me), dst, arrive).start()

            @pl.loop(1, half)
            def _(q):
                one(peer_near(q))

        far()
        near()

    for k, (ref, which, landing) in enumerate(sets):
        @pl.loop(0, chunks)
        def _(g):
            @pl.loop(0, CHUNK // SUB)
            def _(j):
                i = g * (CHUNK // SUB) + j
                ahead = i + SLOTS - 1

                @pl.when(ahead < total)
                def _():
                    load(ref, ahead).start()

                if k < 2:
                    @pl.when(ahead >= total)
                    def _():
                        load(sets[k + 1][0], ahead - total).start()

                load(ref, i).wait()
                slot = lax.rem(i, SLOTS)
                for s in range(SUB):
                    row = i * SUB + s
                    first = column(start_ref[which, pl.ds(row, 1), :])
                    last = column(end_ref[which, pl.ds(row, 1), :] - middle)
                    pieces = []
                    for c in range(samples // LANES):
                        x = buf[slot, s, :, c * LANES:(c + 1) * LANES]
                        tick = ticks[c % (middle // LANES)]
                        keep = tick >= first if c * LANES < middle else tick < last
                        pieces.append(jnp.where(keep, x, jnp.zeros_like(x)))
                    windowed = jnp.concatenate(pieces, axis=1)
                    spec = lax.dot_general(
                        table_ref[...], windowed, (((1,), (1,)), ((), ())),
                        preferred_element_type=f32,
                    )
                    at = pl.multiple_of((j * SUB + s) * waves, waves)
                    for c in range(receivers // LANES):
                        scr[c, pl.ds(at, waves), :] = spec[:, c * LANES:(c + 1) * LANES]

            for w in range(n):
                for c in range(receivers // LANES):
                    re = scr[c, pl.ds(2 * w, CHUNK, stride=waves), :]
                    im = scr[c, pl.ds(2 * w + 1, CHUNK, stride=waves), :]
                    both = jnp.concatenate([re, im], axis=0) * scale_t
                    stage[k, g, w, :, c * LANES:(c + 1) * LANES] = both.astype(bf)

            if k == 0:
                @pl.when(g == 0)
                def _():
                    pl.semaphore_wait(barrier, n - 1)

            arrive = r23_sem.at[k] if k < 2 else r1_sem.at[g]
            there = pl.ds(pl.multiple_of((g * n + me) * PAIR, PAIR), PAIR)
            send(lambda p: stage.at[k, g, p], landing.at[there], send_sem.at[k], arrive, 0)

    scale_f = 1.0 / (n ** 0.5)
    fold = math.frexp(scale_f)[0] == 0.5
    keep_rows = lax.broadcasted_iota(jnp.int32, (PAIR, samples), 0)
    for w in range(0, waves, 2):
        pair = table_ref[w:w + 2, :].astype(f32)
        if fold:
            pair = pair * scale_f
        spread = jnp.concatenate(
            [jnp.broadcast_to(pair[c:c + 1, :], (CHUNK, samples)) for c in range(2)], axis=0
        )
        for s in range(CHUNK):
            here = (keep_rows == s) | (keep_rows == s + CHUNK)
            wide_ref[s, w * CHUNK:(w + 2) * CHUNK, :] = jnp.where(
                here, spread, jnp.zeros_like(spread)
            ).astype(bf)

    drain(r3, r23_sem.at[1])

    @pl.loop(0, chunks * n)
    def _(b):
        rows = pl.ds(pl.multiple_of(b * PAIR, PAIR), PAIR)
        x = r3[rows, :].astype(f32)
        r3s[rows, :] = jnp.concatenate([x[CHUNK:], -x[:CHUNK]], axis=0).astype(bf)

    drain(r2, r23_sem.at[0])
    scale_g = 1.0 / ((n * sources) ** 0.5)
    scale_m = 1.0 / (receivers ** 0.5)
    width = 256
    dot = functools.partial(jnp.dot, preferred_element_type=f32)

    @pl.loop(0, receivers // width)
    def _(b):
        cols = pl.ds(pl.multiple_of(b * width, width), width)
        ct = r2[:, cols].T
        gw[cols, :receivers] = (dot(ct, r3[...]) * scale_g).astype(bf)
        gw[cols, receivers:] = (dot(ct, r3s[...]) * scale_g).astype(bf)

    span = n * PAIR

    @pl.loop(0, chunks)
    def _(g):
        rows = pl.ds(pl.multiple_of(g * span, span), span)
        drain(r1.at[rows], r1_sem.at[g])
        prod = dot(r1[rows, :], gw[...])
        for p in range(n):
            a = prod[p * PAIR:p * PAIR + CHUNK]
            b = prod[p * PAIR + CHUNK:(p + 1) * PAIR]
            re = a[:, :receivers] - b[:, receivers:]
            im = a[:, receivers:] + b[:, :receivers]
            mbuf[g, p] = (jnp.concatenate([re, im], axis=0) * scale_m).astype(bf)
        there = pl.ds(pl.multiple_of((g * n + me) * PAIR, PAIR), PAIR)
        send(lambda p: mbuf.at[g, p], piece.at[there], send_sem.at[3], out_sem.at[g], 1)

    @pl.loop(0, chunks - 1)
    def _(g):
        rows = pl.ds(pl.multiple_of(g * span, span), span)
        drain(piece.at[rows], out_sem.at[g])
        turned[...] = piece[rows, :].T

        @pl.loop(0, CHUNK)
        def _(s):
            early_ref[g * CHUNK + s] = inverse(turned[...], wide_ref[s], fold, scale_f)

    rows = pl.ds((chunks - 1) * span, span)
    drain(piece.at[rows], out_sem.at[chunks - 1])
    last_ref[...] = piece[rows, :].T
    for k in range(3):
        drain(stage.at[k, :, pl.ds(0, n - 1)], send_sem.at[k])
    drain(mbuf.at[:, pl.ds(0, n - 1)], send_sem.at[3])


def inverse(turned, wide, fold, scale):
    timed = jnp.dot(turned, wide, preferred_element_type=jnp.float32)
    if not fold:
        timed = timed * scale
    return timed.astype(jnp.bfloat16)


def write_kernel(n, early_ref, last_ref, wide_ref, out_ref, tail, early_sem, tail_sem):
    early = early_ref.shape[0]
    scale = 1.0 / (n ** 0.5)
    fold = math.frexp(scale)[0] == 0.5

    def bulk(g):
        at = pl.ds(g * CHUNK, CHUNK)
        return pltpu.make_async_copy(early_ref.at[at], out_ref.at[at], early_sem.at[g])

    for g in range(early // CHUNK):
        bulk(g).start()

    def rest(s):
        return pltpu.make_async_copy(tail.at[s], out_ref.at[early + s], tail_sem.at[s])

    @pl.loop(0, CHUNK)
    def _(s):
        tail[s] = inverse(last_ref[...], wide_ref[s], fold, scale)
        rest(s).start()

    for g in range(early // CHUNK):
        bulk(g).wait()

    @pl.loop(0, CHUNK)
    def _(s):
        rest(s).wait()


def spectrum(traces, start, finish, table, count):
    sources, receivers, samples = traces.shape
    times = jnp.arange(samples, dtype=jnp.int32)
    inside = (times >= start[:, :, None]) & (times < finish[:, :, None])
    windowed = jnp.where(inside, traces, jnp.zeros_like(traces))
    flat = windowed.reshape(sources * receivers, samples)
    spec = lax.dot_general(
        table, flat, (((1,), (1,)), ((), ())), preferred_element_type=jnp.float32
    )
    spec = spec * (1.0 / jnp.sqrt(jnp.float32(samples)))
    return spec.astype(jnp.bfloat16).reshape(count, 2, sources, receivers)


def correlate(first, second):
    swapped = jnp.stack([first[:, 1], -first[:, 0]], axis=1)
    left = jnp.stack([first, swapped], axis=1)
    cross = jnp.einsum("fkcsr,fcur->fksu", left, second, preferred_element_type=jnp.float32)
    cross = cross * (1.0 / jnp.sqrt(jnp.float32(first.shape[3])))
    return cross.astype(jnp.bfloat16)


def convolve(cross, third):
    right = jnp.stack(
        [
            jnp.stack([third[:, 0], -third[:, 1]], axis=1),
            jnp.stack([third[:, 1], third[:, 0]], axis=1),
        ],
        axis=1,
    )
    multiple = jnp.einsum("fcsu,fkcur->fksr", cross, right, preferred_element_type=jnp.float32)
    multiple = multiple * (1.0 / jnp.sqrt(jnp.float32(third.shape[2])))
    return multiple.astype(jnp.bfloat16)


def plain_on_device(primary_one, primary_two, primary_three, window_start, window_end):
    samples = primary_one.shape[2]
    count = F_DEV * lax.axis_size("freq")
    table = make_table(count, samples)
    spec_one = spectrum(primary_one, window_start[0], window_end[0], table, count)
    spec_two = spectrum(primary_two, window_start[1], window_end[1], table, count)
    spec_three = spectrum(primary_three, window_start[2], window_end[2], table, count)
    first, second, third = (
        lax.all_to_all(spec_one, "freq", split_axis=0, concat_axis=2, tiled=True),
        lax.all_to_all(spec_two, "freq", split_axis=0, concat_axis=2, tiled=True),
        lax.all_to_all(spec_three, "freq", split_axis=0, concat_axis=2, tiled=True),
    )
    cross = correlate(first, second)
    multiple = convolve(cross, third)
    piece = lax.all_to_all(multiple, "freq", split_axis=2, concat_axis=0, tiled=True)
    waves, parts, sources, receivers = piece.shape
    flat = piece.reshape(waves * parts, sources * receivers)
    timed = lax.dot_general(
        flat, table, (((0,), (0,)), ((), ())), preferred_element_type=jnp.float32
    )
    timed = timed * (1.0 / jnp.sqrt(jnp.float32(count)))
    return timed.astype(jnp.bfloat16).reshape(sources, receivers, samples)


def on_device(primary_one, primary_two, primary_three, window_start, window_end):
    sources, receivers, samples = primary_one.shape
    n = lax.axis_size("freq")
    fits = sources * receivers * samples * 2 <= 16 << 20 and n * sources <= 512 and samples <= 512
    if not fits or n > 16 or n % 2 or sources % CHUNK or receivers % 256 or samples % (2 * LANES):
        return plain_on_device(
            primary_one, primary_two, primary_three, window_start, window_end
        )
    table = host_table(F_DEV * n, samples)
    bf = jnp.bfloat16
    chunks = sources // CHUNK
    rows = chunks * n * PAIR
    span = n * PAIR
    vmem = pl.BlockSpec(memory_space=pltpu.VMEM)
    hbm = pl.BlockSpec(memory_space=pl.ANY)
    early, last, wide = pl.pallas_call(
        functools.partial(exchange_kernel, n),
        out_shape=(
            pltpu.VMEM((sources - CHUNK, receivers, samples), bf),
            pltpu.VMEM((receivers, span), bf),
            pltpu.VMEM((CHUNK, span, samples), bf),
        ),
        in_specs=[hbm] * 6,
        out_specs=(vmem, vmem, vmem),
        scratch_shapes=[
            pltpu.VMEM(window_start.shape, jnp.int32),
            pltpu.VMEM(window_end.shape, jnp.int32),
            pltpu.VMEM(table.shape, bf),
            pltpu.VMEM((SLOTS, SUB, receivers, samples), bf),
            pltpu.VMEM((receivers // LANES, CHUNK * 2 * n, LANES), jnp.float32),
            pltpu.VMEM((3, chunks, n, PAIR, receivers), bf),
            pltpu.VMEM((rows, receivers), bf),
            pltpu.VMEM((rows, receivers), bf),
            pltpu.VMEM((rows, receivers), bf),
            pltpu.VMEM((rows, receivers), bf),
            pltpu.VMEM((receivers, 2 * receivers), bf),
            pltpu.VMEM((chunks, n, PAIR, receivers), bf),
            pltpu.VMEM((rows, receivers), bf),
            pltpu.VMEM((receivers, span), bf),
            pltpu.SemaphoreType.DMA((SLOTS,)),
            pltpu.SemaphoreType.DMA((3,)),
            pltpu.SemaphoreType.DMA((4,)),
            pltpu.SemaphoreType.DMA((chunks,)),
            pltpu.SemaphoreType.DMA((2,)),
            pltpu.SemaphoreType.DMA((chunks,)),
        ],
        compiler_params=pltpu.CompilerParams(
            collective_id=0, has_side_effects=True, vmem_limit_bytes=40 << 20,
        ),
        name="exchange",
    )(primary_one, primary_two, primary_three, window_start, window_end, table)
    return pl.pallas_call(
        functools.partial(write_kernel, n),
        out_shape=jax.ShapeDtypeStruct(primary_one.shape, bf),
        in_specs=[vmem, vmem, vmem],
        out_specs=hbm,
        scratch_shapes=[
            pltpu.VMEM((CHUNK, receivers, samples), bf),
            pltpu.SemaphoreType.DMA((chunks,)),
            pltpu.SemaphoreType.DMA((CHUNK,)),
        ],
        compiler_params=pltpu.CompilerParams(vmem_limit_bytes=20 << 20),
        name="write",
    )(early, last, wide)


def solution(mesh):
    return jax.shard_map(
        on_device,
        mesh=mesh,
        in_specs=(
            P(("groups", "freq"), None, None),
            P(("groups", "freq"), None, None),
            P(("groups", "freq"), None, None),
            P(None, ("groups", "freq"), None),
            P(None, ("groups", "freq"), None),
        ),
        out_specs=P(("groups", "freq"), None, None),
        check_vma=False,
    )
```
